32 devices in a mesh: dp: 4 (over z), vp: 8 (over y, x, core).
Axes of the slice: x: 2, y: 2, z: 4, core: 2. Of those that a mesh axis runs over, the one named last changes fastest.
Arguments:
- hidden: bfloat16 [8, 1024, 896], P('dp')
- targets: int32 [8, 1024], P('dp')
- loss_mask: int32 [8, 1024], P('dp')
- norm_gain: float32 [896], replicated
- emb_table: bfloat16 [152000, 896], P('vp')
Outputs:
- output 1: float32 [], replicated
- output 2: float32 [8, 1024, 896], P('dp')
- output 3: float32 [152000, 896], P('vp')
- output 4: float32 [896], replicated
All inputs are finite; a program needn't handle non-finite values.
Results may differ from the reference program's by a relative error of at most 0.001.
Values sent between devices are 32-bit elements.
A program may use at most 1 GiB of HBM per device.

```python
import math
import jax
import jax.numpy as jnp
from jax import lax

WIDTH = 896
VOCAB_REAL = 151936
PAD_ROWS = 64
SAMPLES = 8
SEQ_LEN = 1024
ROW_BLOCK = 16
VOCAB_ROWS = VOCAB_REAL + PAD_ROWS
SOFT_CAP = 30.0
NORM_EPS = 1e-6
EMBED_STD = 23.0 / math.sqrt(WIDTH)


def draw_mask_targets(index_key):
    key_len, key_pos, key_tgt = jax.random.split(index_key, 3)
    win_len = SEQ_LEN // 2
    suffix_len = jax.random.randint(key_len, (SAMPLES,), 1, win_len + 1)
    suffix_len = suffix_len.at[0].set(win_len)
    suffix_pos = jax.random.randint(key_pos, (SAMPLES,), 0, SEQ_LEN - suffix_len + 1)
    positions = jnp.arange(SEQ_LEN)[None, :]
    inside = (positions >= suffix_pos[:, None]) & (positions < (suffix_pos + suffix_len)[:, None])
    loss_mask = inside.astype(jnp.int32)
    targets = jax.random.randint(key_tgt, (SAMPLES, SEQ_LEN), 0, VOCAB_REAL)
    return targets, loss_mask


def setup_inputs(seed: int = 0) -> dict:
    base_key = jax.random.key(seed)
    key_hid, key_gain, key_table, key_idx = jax.random.split(base_key, 4)
    hidden = jax.random.normal(key_hid, (SAMPLES, SEQ_LEN, WIDTH), jnp.float32).astype(jnp.bfloat16)
    norm_gain = 0.3 * jax.random.normal(key_gain, (WIDTH,), jnp.float32)
    emb_table = (EMBED_STD * jax.random.normal(key_table, (VOCAB_ROWS, WIDTH), jnp.float32)).astype(jnp.bfloat16)
    targets, loss_mask = draw_mask_targets(key_idx)
    return {'hidden': hidden, 'targets': targets, 'loss_mask': loss_mask, 'norm_gain': norm_gain, 'emb_table': emb_table}


def reference(hidden, targets, loss_mask, norm_gain, emb_table):
    num_blocks = SAMPLES * SEQ_LEN // ROW_BLOCK
    hid_blocks = hidden.reshape(num_blocks, ROW_BLOCK, WIDTH)
    tgt_blocks = targets.reshape(num_blocks, ROW_BLOCK)
    mask_blocks = loss_mask.reshape(num_blocks, ROW_BLOCK).astype(jnp.float32)
    mask_count = jnp.sum(mask_blocks)
    gain_vec = 1.0 + norm_gain
    col_ids = jnp.arange(VOCAB_ROWS)
    real_cols = (col_ids < VOCAB_REAL)[None, :]

    def block_step(acc_state, block_in):
        table_acc, loss_acc = acc_state
        hid_blk, tgt_blk, mask_blk = block_in
        hid_f32 = hid_blk.astype(jnp.float32)
        inv_rms = lax.rsqrt(jnp.mean(hid_f32 * hid_f32, axis=-1, keepdims=True) + NORM_EPS)
        normed = hid_f32 * inv_rms
        normed_bf = (normed * gain_vec).astype(jnp.bfloat16)
        logits = jnp.dot(normed_bf, emb_table.T, preferred_element_type=jnp.float32)
        tanh_vals = jnp.tanh(logits / SOFT_CAP)
        capped = jnp.where(real_cols, SOFT_CAP * tanh_vals, -jnp.inf)
        log_norm = jax.nn.logsumexp(capped, axis=-1)
        is_target = col_ids[None, :] == tgt_blk[:, None]
        tgt_logit = jnp.sum(jnp.where(is_target, capped, 0.0), axis=-1)
        prob_vals = jnp.exp(capped - log_norm[:, None])
        logit_grad = ((prob_vals - is_target.astype(jnp.float32)) * (1.0 - tanh_vals * tanh_vals) * (mask_blk / mask_count)[:, None]).astype(jnp.bfloat16)
        norm_grad = jnp.dot(logit_grad, emb_table, preferred_element_type=jnp.float32)
        table_acc = table_acc + jnp.dot(logit_grad.T, normed_bf, preferred_element_type=jnp.float32)
        loss_acc = loss_acc + jnp.sum((log_norm - tgt_logit) * mask_blk)
        scaled_grad = norm_grad * gain_vec
        hid_grad = inv_rms * scaled_grad - hid_f32 * (inv_rms ** 3) * jnp.mean(scaled_grad * hid_f32, axis=-1, keepdims=True)
        gain_part = jnp.sum(norm_grad * normed, axis=0)
        return (table_acc, loss_acc), (hid_grad, gain_part)

    start_state = (jnp.zeros((VOCAB_ROWS, WIDTH), jnp.float32), jnp.zeros((), jnp.float32))
    (table_grad, loss_sum), (hid_grads, gain_parts) = lax.scan(block_step, start_state, (hid_blocks, tgt_blocks, mask_blocks))
    return (loss_sum / mask_count, hid_grads.reshape(SAMPLES, SEQ_LEN, WIDTH), table_grad, jnp.sum(gain_parts, axis=0))
```

```python
import functools
import math

import jax
import jax.numpy as jnp
from jax import lax
from jax.experimental import pallas as pl
from jax.experimental.pallas import tpu as pltpu
from jax.sharding import PartitionSpec as P

SOFT_CAP = 30.0
NORM_EPS = 1e-6
PAD_ROWS = 64
MAX_RUN = 512
LOG2E = math.log2(math.e)
TB = 256
VT = 760
F32 = jnp.float32
BF16 = jnp.bfloat16
MESH = pl.DeviceIdType.MESH
VMEM_LIMIT = 63 * 1024 * 1024


def _nt(a, b):
    return lax.dot_general(a, b, (((1,), (1,)), ((), ())), preferred_element_type=F32)


def _tn(a, b):
    return lax.dot_general(a, b, (((0,), (0,)), ((), ())), preferred_element_type=F32)


def _fwd_kernel(info, e_ref, u_ref, y_ref, s_ref, t_ref, *e_out):
    step = pl.program_id(0)
    nblk = info[0]
    row0 = step * VT
    nvalid = info[1] - row0

    @pl.when(step == 0)
    def _():
        s_ref[...] = jnp.zeros_like(s_ref)
        t_ref[...] = jnp.zeros_like(t_ref)

    def run(first, count):
        zs = [_nt(e_ref[...], u_ref[(first + k) * TB:(first + k + 1) * TB, :]) for k in range(count)]
        rid = lax.broadcasted_iota(jnp.int32, (VT, TB), 0)
        for k in range(count):
            cols = slice((first + k) * TB, (first + k + 1) * TB)
            t = jnp.tanh(zs[k] * (1.0 / SOFT_CAP))
            ex = jnp.exp2(t * (SOFT_CAP * LOG2E) - (SOFT_CAP * LOG2E))
            ex = jnp.where(rid < nvalid, ex, 0.0)
            s_ref[:, cols] += jnp.sum(ex, axis=0, keepdims=True)
            hit = rid == (y_ref[:, cols] - row0)
            t_ref[:, cols] += jnp.sum(jnp.where(hit, t, 0.0), axis=0, keepdims=True)
            e_out[first + k][...] = ex * (1.0 - t * t)

    pl.when(nblk == 1)(lambda: run(0, 1))
    pl.when(nblk >= 2)(lambda: run(0, 2))
    pl.when(nblk == 3)(lambda: run(2, 1))
    pl.when(nblk == 4)(lambda: run(2, 2))


def _own_kernel(info, e_ref, u_ref, y_ref, a_ref, b_ref, *rest):
    e_in, (du_ref, de_ref, g_ref) = rest[:4], rest[4:]
    step = pl.program_id(0)
    nblk = info[0]
    row0 = step * VT

    @pl.when(step == 0)
    def _():
        du_ref[...] = jnp.zeros_like(du_ref)

    def run(first, count, init):
        rid = lax.broadcasted_iota(jnp.int32, (VT, TB), 0)
        for k in range(count):
            cols = slice((first + k) * TB, (first + k + 1) * TB)
            g = e_in[first + k][...] * a_ref[:, cols]
            g = jnp.where(rid == (y_ref[:, cols] - row0), g - b_ref[:, cols], g)
            g_ref[:, k * TB:(k + 1) * TB] = g.astype(BF16)
        gb = g_ref[:, :count * TB]
        rows = slice(first * TB, (first + count) * TB)
        prod = jnp.dot(gb, u_ref[rows, :], preferred_element_type=F32)
        if init:
            de_ref[...] = prod
        else:
            de_ref[...] += prod
        du_ref[rows, :] += _tn(gb, e_ref[...])

    pl.when(nblk == 1)(lambda: run(0, 1, True))
    pl.when(nblk >= 2)(lambda: run(0, 2, True))
    pl.when(nblk == 3)(lambda: run(2, 1, False))
    pl.when(nblk == 4)(lambda: run(2, 2, False))


def _other_kernel(info, e_ref, u_ref, st_ref, din_ref, dout_ref):
    step = pl.program_id(0)
    nblk = info[0]
    row0 = step * VT
    nvalid = info[1] - row0
    ybase = (info[2] + row0).astype(F32)
    dout_ref[...] = din_ref[...]

    def run(base, count):
        def cols(k):
            return pl.ds(pl.multiple_of(base + k * TB, TB), TB)

        rid = lax.broadcasted_iota(jnp.int32, (VT, TB), 0)
        rid_f = rid.astype(F32)
        zs = [_nt(e_ref[...], u_ref[cols(k), :]) for k in range(count)]
        gs = []
        for k in range(count):
            lse2 = st_ref[0:1, cols(k)]
            w = st_ref[1:2, cols(k)]
            yl = st_ref[2:3, cols(k)] - ybase
            t = jnp.tanh(zs[k] * (1.0 / SOFT_CAP))
            p = jnp.exp2(t * (SOFT_CAP * LOG2E) - lse2)
            p = jnp.where(rid_f == yl, p - 1.0, p)
            g = (p * (1.0 - t * t)) * w
            gs.append(jnp.where(rid < nvalid, g, 0.0).astype(BF16))
        g = jnp.concatenate(gs, axis=1) if count > 1 else gs[0]
        dout_ref[...] += jnp.dot(g, u_ref[pl.ds(pl.multiple_of(base, TB), count * TB), :], preferred_element_type=F32)

    def body(b, carry):
        run(b * (4 * TB), 4)
        return carry

    full = nblk // 4
    lax.fori_loop(0, full, body, 0)
    left = nblk - 4 * full
    base = full * (4 * TB)
    pl.when(left >= 2)(lambda: run(base, 2))
    pl.when(left % 2 == 1)(lambda: run(base + (left - 1) * TB, 1))


def _stats_kernel(dp_size, vp_size, s_ref, t_ref, ym_ref, out_ref, mine, got, packed, send1, recv1, send2, recv2):
    dp, vp = lax.axis_index('dp'), lax.axis_index('vp')
    barrier = pltpu.get_barrier_semaphore()
    for j in range(1, vp_size):
        pl.semaphore_signal(barrier, inc=1, device_id=(dp, lax.rem(vp + j, vp_size)), device_id_type=MESH)
    for j in range(1, dp_size):
        pl.semaphore_signal(barrier, inc=1, device_id=(lax.rem(dp + j, dp_size), vp), device_id_type=MESH)
    mine[0:8, :] = jnp.concatenate([s_ref[:, k * 128:(k + 1) * 128] for k in range(8)], axis=0)
    mine[8:16, :] = jnp.concatenate([t_ref[:, k * 128:(k + 1) * 128] for k in range(8)], axis=0)
    pl.semaphore_wait(barrier, vp_size + dp_size - 2)
    copies = []
    for j in range(1, vp_size):
        copy = pltpu.make_async_remote_copy(
            src_ref=mine, dst_ref=got.at[j - 1], send_sem=send1.at[j - 1], recv_sem=recv1.at[j - 1],
            device_id=(dp, lax.rem(vp + j, vp_size)), device_id_type=MESH)
        copy.start()
        copies.append(copy)
    total = mine[...]
    for j, copy in enumerate(copies):
        copy.wait()
    parts = [total] + [got[j] for j in range(vp_size - 1)]
    total = jnp.zeros_like(total)
    for v in range(vp_size):
        part = jnp.zeros_like(total)
        for j in range(vp_size):
            sender = lax.rem(vp - j + vp_size, vp_size)
            part = jnp.where(sender == v, parts[j], part)
        total = total + part
    s_tot, t_tot = total[0:8, :], total[8:16, :]
    packed[0, 0:8, :] = s_tot
    packed[0, 8:16, :] = t_tot
    packed[0, 16:32, :] = ym_ref[...]
    copies = []
    for j in range(1, dp_size):
        copy = pltpu.make_async_remote_copy(
            src_ref=packed.at[0], dst_ref=packed.at[j], send_sem=send2.at[j - 1], recv_sem=recv2.at[j - 1],
            device_id=(lax.rem(dp - j + dp_size, dp_size), vp), device_id_type=MESH)
        copy.start()
        copies.append(copy)
    for copy in copies:
        copy.wait()
    out_ref[...] = packed[...]


def _exchange_stats(dp_size, vp_size, s_part, t_part, ym):
    return pl.pallas_call(
        functools.partial(_stats_kernel, dp_size, vp_size),
        out_shape=jax.ShapeDtypeStruct((dp_size, 32, 128), F32),
        in_specs=[pl.BlockSpec(memory_space=pltpu.VMEM)] * 3,
        out_specs=pl.BlockSpec(memory_space=pltpu.VMEM),
        scratch_shapes=[
            pltpu.VMEM((16, 128), F32),
            pltpu.VMEM((vp_size - 1, 16, 128), F32),
            pltpu.VMEM((dp_size, 32, 128), F32),
            pltpu.SemaphoreType.DMA((vp_size - 1,)),
            pltpu.SemaphoreType.DMA((vp_size - 1,)),
            pltpu.SemaphoreType.DMA((dp_size - 1,)),
            pltpu.SemaphoreType.DMA((dp_size - 1,)),
        ],
        compiler_params=pltpu.CompilerParams(collective_id=0, has_side_effects=True),
        name='stats_exchange',
    )(s_part, t_part, ym)


def _compact_kernel(others, cap, info, u_hbm, st_ref, u_out, st_out, src, buf, sem):
    step = 64
    own = 2 * MAX_RUN
    copies = [pltpu.make_async_copy(u_hbm.at[info[4 + j]], src.at[j, pl.ds(step, own)], sem.at[j]) for j in range(others)]
    for copy in copies:
        copy.start()
    edge = jnp.zeros((step, buf.shape[1]), F32)

    def clear(i, carry):
        buf[pl.ds(pl.multiple_of(i * step, step), step), :] = edge
        return carry

    lax.fori_loop(0, info[0] * (TB // step), clear, 0)
    off = 0
    acc = jnp.zeros(st_out.shape, F32)
    for j in range(others):
        src[j, 0:step, :] = edge
        src[j, step + own:2 * step + own, :] = edge
        rows = jnp.concatenate([st_ref[j], jnp.zeros((8, cap - own), F32)], axis=1)
        acc = acc + pltpu.roll(rows, off, 1)
        copies[j].wait()

        def move(c, carry, j=j, off=off):
            first = step + c * step - off
            low = (first // 8) * 8
            part = src[j, pl.ds(pl.multiple_of(low, 8), step + 8), :]
            part = pltpu.roll(part, lax.rem(step + 8 - (first - low), step + 8), 0)[:step]
            buf[pl.ds(pl.multiple_of(c * step, step), step), :] += part
            return carry

        end = off + info[1 + j]
        lax.fori_loop(off // step, (end + step - 1) // step, move, 0)
        off = end
    st_out[...] = acc

    def conv(i, carry):
        rows = pl.ds(pl.multiple_of(i * TB, TB), TB)
        u_out[rows, :] = buf[rows, :].astype(BF16)
        return carry

    lax.fori_loop(0, info[0], conv, 0)


def solution(mesh):
    dp_size, vp_size = mesh.shape['dp'], mesh.shape['vp']
    others = dp_size - 1

    def shard_fn(hidden, targets, loss_mask, norm_gain, emb_table):
        samples, seq_len, width = hidden.shape
        own_rows = emb_table.shape[0]
        vocab_real = own_rows * vp_size - PAD_ROWS
        dp, vp = lax.axis_index('dp'), lax.axis_index('vp')
        row_start = vp * own_rows
        num_tok = samples * seq_len
        cap_own = samples * MAX_RUN
        cap_oth = others * cap_own
        cap_buf = cap_oth + cap_own
        grid = own_rows // VT

        pos = jnp.arange(seq_len)
        lens = jnp.sum(loss_mask, axis=1)
        starts = jnp.min(jnp.where(loss_mask > 0, pos[None, :], seq_len), axis=1)
        slot = jnp.arange(cap_own)
        in_first = slot < lens[0]
        idx = jnp.where(in_first, starts[0] + slot, seq_len + starts[1] + slot - lens[0])
        own_count = lens[0] + lens[1]
        valid = slot < own_count
        idx = jnp.where(valid, idx, 0)
        h_c = jnp.where(valid[:, None], jnp.take(hidden.reshape(num_tok, width), idx, axis=0).astype(F32), 0.0)
        y_c = jnp.take(targets.reshape(num_tok), idx)
        inv_rms = lax.rsqrt(jnp.mean(h_c * h_c, axis=-1, keepdims=True) + NORM_EPS)
        normed = h_c * inv_rms
        gain_vec = 1.0 + norm_gain
        u_own = (normed * gain_vec).astype(BF16)
        share = cap_own // vp_size
        mine = lax.dynamic_slice_in_dim(u_own, vp * share, share, 0).astype(F32)
        u_all = lax.all_gather(mine, ('dp', 'vp'), axis=0, tiled=True).reshape(dp_size, cap_own, width)

        nblk_own = (own_count + TB - 1) // TB
        info = jnp.stack([nblk_own, vocab_real - row_start]).astype(jnp.int32)
        y_loc = (y_c - row_start).astype(jnp.int32)[None, :]

        def eblk(k):
            return pl.BlockSpec((VT, TB), lambda i, n, k=k: (jnp.where(k < n[0], i, 0), 0))

        tile = pl.BlockSpec((VT, width), lambda i, n: (i, 0))
        whole = pl.BlockSpec(memory_space=pltpu.VMEM)
        nb = cap_own // TB
        flops = 2 * own_rows * width
        s_part, t_part, *e_blk = pl.pallas_call(
            _fwd_kernel,
            grid_spec=pltpu.PrefetchScalarGridSpec(
                num_scalar_prefetch=1, grid=(grid,),
                in_specs=[tile, whole, whole],
                out_specs=[pl.BlockSpec((1, cap_own), lambda i, n: (0, 0))] * 2 + [eblk(k) for k in range(nb)]),
            out_shape=[jax.ShapeDtypeStruct((1, cap_own), F32)] * 2
            + [jax.ShapeDtypeStruct((own_rows, TB), F32)] * nb,
            compiler_params=pltpu.CompilerParams(dimension_semantics=('arbitrary',), vmem_limit_bytes=VMEM_LIMIT),
            cost_estimate=pl.CostEstimate(flops=flops * 768, bytes_accessed=own_rows * width * 6, transcendentals=0),
            name='own_forward',
        )(info, emb_table, u_own, y_loc)

        ym = jnp.concatenate([y_c.astype(F32).reshape(8, 128), valid.astype(F32).reshape(8, 128)], axis=0)
        stats = _exchange_stats(dp_size, vp_size, s_part, t_part, ym).reshape(dp_size, 4, cap_own)
        s_all, t_all, y_all, m_all = stats[:, 0], stats[:, 1], stats[:, 2], stats[:, 3]
        counts = jnp.sum(m_all, axis=1)
        mask_count = jnp.sum(counts)
        log_s = jnp.log(jnp.where(m_all > 0, s_all, 1.0))
        lse = SOFT_CAP + log_s
        mean_loss_rot = jnp.sum((lse - SOFT_CAP * t_all) * m_all, axis=1)
        loss_dp = jnp.roll(mean_loss_rot, dp)
        mean_loss = (((loss_dp[0] + loss_dp[1]) + loss_dp[2]) + loss_dp[3]) / mask_count
        w_all = m_all / mask_count

        a_own = (w_all[0] * jnp.exp(-log_s[0]))[None, :]
        b_own = (w_all[0] * (1.0 - t_all[0] * t_all[0]))[None, :]
        du, de = pl.pallas_call(
            _own_kernel,
            grid_spec=pltpu.PrefetchScalarGridSpec(
                num_scalar_prefetch=1, grid=(grid,),
                in_specs=[tile, whole, whole, whole, whole] + [eblk(k) for k in range(nb)],
                out_specs=[pl.BlockSpec((cap_own, width), lambda i, n: (0, 0)), tile],
                scratch_shapes=[pltpu.VMEM((VT, 2 * TB), BF16)]),
            out_shape=[jax.ShapeDtypeStruct((cap_own, width), F32), jax.ShapeDtypeStruct((own_rows, width), F32)],
            compiler_params=pltpu.CompilerParams(dimension_semantics=('arbitrary',), vmem_limit_bytes=VMEM_LIMIT),
            cost_estimate=pl.CostEstimate(flops=flops * 2 * 768, bytes_accessed=own_rows * width * 10, transcendentals=0),
            name='own_backward',
        )(info, emb_table, u_own, y_loc, a_own, b_own, *e_blk)
        du_sum = lax.psum(du, 'vp')

        cnt = counts.astype(jnp.int32)
        oth_count = cnt[1] + cnt[2] + cnt[3]
        nblk_oth = (oth_count + TB - 1) // TB
        order = [lax.rem(dp + j, dp_size).astype(jnp.int32) for j in range(1, dp_size)]
        cinfo = jnp.stack([nblk_oth, cnt[1], cnt[2], cnt[3]] + order).astype(jnp.int32)
        zero = jnp.zeros_like(w_all[1:])
        st_in = jnp.stack([lse[1:] * LOG2E, w_all[1:], y_all[1:] - row_start.astype(F32)] + [zero] * 5, axis=1)
        st_in = jnp.where(m_all[1:, None, :] > 0, st_in, 0.0)
        u_oth, st_oth = pl.pallas_call(
            functools.partial(_compact_kernel, others, cap_buf),
            in_specs=[pl.BlockSpec(memory_space=pltpu.SMEM), pl.BlockSpec(memory_space=pl.ANY), whole],
            out_specs=[whole, whole],
            out_shape=[jax.ShapeDtypeStruct((cap_oth, width), BF16), jax.ShapeDtypeStruct((8, cap_buf), F32)],
            scratch_shapes=[pltpu.VMEM((others, cap_own + 128, width), F32), pltpu.VMEM((cap_oth, width), F32),
                            pltpu.SemaphoreType.DMA((others,))],
            compiler_params=pltpu.CompilerParams(vmem_limit_bytes=VMEM_LIMIT),
            name='compact',
        )(cinfo, u_all, st_in)
        oinfo = jnp.stack([nblk_oth, vocab_real - row_start, 0]).astype(jnp.int32)
        table_grad = pl.pallas_call(
            _other_kernel,
            grid_spec=pltpu.PrefetchScalarGridSpec(
                num_scalar_prefetch=1, grid=(grid,),
                in_specs=[tile, whole, whole, tile],
                out_specs=tile),
            out_shape=jax.ShapeDtypeStruct((own_rows, width), F32),
            input_output_aliases={4: 0},
            compiler_params=pltpu.CompilerParams(dimension_semantics=('arbitrary',), vmem_limit_bytes=VMEM_LIMIT),
            cost_estimate=pl.CostEstimate(flops=flops * 2 * 1536, bytes_accessed=own_rows * width * 10, transcendentals=0),
            name='other_tokens',
        )(oinfo, emb_table, u_oth, st_oth, de)

        table_grad, du_sum = lax.optimization_barrier((table_grad, du_sum))
        scaled = du_sum * gain_vec
        dh_c = inv_rms * scaled - h_c * (inv_rms ** 3) * jnp.mean(scaled * h_c, axis=-1, keepdims=True)
        gain_grad = lax.psum(jnp.sum(du_sum * normed, axis=0), 'dp')
        back = jnp.where(jnp.arange(samples)[:, None] == 0, pos[None, :] - starts[0], pos[None, :] - starts[1] + lens[0])
        inside = loss_mask > 0
        back = jnp.where(inside, back, 0).reshape(num_tok)
        hid_grad = jnp.where(inside[:, :, None], jnp.take(dh_c, back, axis=0).reshape(samples, seq_len, width), 0.0)
        return mean_loss, hid_grad, table_grad, gain_grad

    return jax.shard_map(shard_fn, mesh=mesh, in_specs=(P('dp'), P('dp'), P('dp'), P(), P('vp')),
                         out_specs=(P(), P('dp'), P('vp'), P()), check_vma=False)
```
